32 devices in a mesh: freq: 4 (over z), strip: 8 (over y, x, core).
Axes of the slice: x: 2, y: 2, z: 4, core: 2. Of those that a mesh axis runs over, the one named last changes fastest.
Arguments:
- receiver_field: float32 [2, 4, 64, 512], P(None, 'freq', 'strip'), may hold values from -17 to 17
- source_field: float32 [2, 4, 64, 512], P(None, 'freq', 'strip'), may hold values from -4 to 4
- velocity_class: int32 [64, 512], P('strip'), may hold values from 0 to 7
- filters: float32 [4, 8, 2, 9], P('freq'), may hold values from -0.8 to 0.8
- point_spread: float32 [16, 2, 15, 15], replicated, may hold values from -0.05 to 1
- spread_index: int32 [8, 4], replicated, may hold values from 0 to 15
Outputs:
- migrated: float32 [64, 2, 512], P('strip', None, 'freq')
- reflectivity: float32 [64, 2, 512], P('strip', None, 'freq')
- misfit: float32 [], replicated
The draws below stay inside these ranges and needn't reach their ends.
All inputs are finite; a program needn't handle non-finite values.
Results may differ from the reference program's by a relative error of at most 0.0003.
Values sent between devices are 32-bit elements; how exact they have to be, the bound alone decides.
A program may use at most 64 MiB of HBM per device.

```python
import math
import jax
import jax.numpy as jnp
from jax import lax

ROWS = 8
BCOLS = 128
STEPS = 2
NCLASS = 8
PSF_SIDE = 15
NPSF = 16
PASSES = 2
NX = 64
NY = 512
NF = 4
BRICKS_X = 8
BRICKS_Y = 4


def draw_receiver_field(key, part):
    shape = (2, NF, NX, NY)
    across = jnp.arange(NY, dtype=jnp.float32) / NY
    raw = jax.random.truncated_normal(key, -4.0, 4.0, shape, jnp.float32)
    return raw * jnp.power(3.0, across)[None, None, None, :]


def draw_filters(key, part):
    first, second, third = jax.random.split(jax.random.fold_in(key, 17), 3)
    shape = (NF, NCLASS, 2, 9)
    taps = 0.15 * jax.random.truncated_normal(first, -4.0, 4.0, shape, jnp.float32)
    phase = jax.random.uniform(second, (NF, NCLASS), jnp.float32, -math.pi, math.pi)
    length = jax.random.uniform(third, (NF, NCLASS), jnp.float32, 0.6, 0.8)
    center = jnp.stack([length * jnp.cos(phase), length * jnp.sin(phase)], axis=2)
    return taps.at[:, :, :, 4].set(center)


def draw_point_spread(key, part):
    first, second = jax.random.split(jax.random.fold_in(key, 29), 2)
    shape = (NPSF, STEPS, PSF_SIDE, PSF_SIDE)
    raw = 0.012 * jax.random.truncated_normal(first, -4.0, 4.0, shape, jnp.float32)
    center = jax.random.uniform(second, (NPSF,), jnp.float32, 0.8, 1.0)
    return raw.at[:, 0, PSF_SIDE // 2, PSF_SIDE // 2].set(center)


def with_ends(array, own_key, low, top_value):
    longest = array.shape.index(max(array.shape))
    spots = []
    for shift in (0, 1):
        where = [jax.random.randint(jax.random.fold_in(own_key, axis), (), 0, length) for axis, length in enumerate(array.shape)]
        where[longest] = (where[longest] + shift) % array.shape[longest]
        spots.append(tuple(where))
    return array.at[spots[0]].set(low).at[spots[1]].set(top_value)


def block_scale(rng, extent, shards, smallest, top_value):
    def one(position, shards_of):
        steps = jax.random.uniform(jax.random.fold_in(jax.random.fold_in(rng, 6), position), (shards_of,), jnp.float32, smallest / len(shards), top_value / len(shards))
        return jnp.repeat(jnp.exp(steps), extent[position] // shards_of).reshape((-1,) + (1,) * (len(extent) - position - 1))

    factor_of = one(*shards[0])
    for cut in shards[1:]:
        factor_of = factor_of * one(*cut)
    return factor_of


def bell_draw(own_key, dims, spread, most, pieces=(), held_as=jnp.bfloat16):
    entries = jax.random.normal(own_key, dims, jnp.float32) * spread
    if len(pieces) > 0:
        entries = block_scale(own_key, dims, pieces, -0.22, 0.18) * entries
    return jnp.clip(entries, min=-most, max=most).astype(held_as)


def setup_inputs(seed: int = 0) -> dict:
    keys = jax.random.split(jax.random.key(seed), 7)
    return {
        "receiver_field": draw_receiver_field(jax.random.fold_in(keys[6], 71), 0),
        "source_field": bell_draw(keys[1], (2, NF, NX, NY), 1.0, 4.0, ((1, 4), (2, 8)), jnp.float32),
        "velocity_class": with_ends(jax.random.randint(keys[2], (NX, NY), 0, NCLASS), jax.random.fold_in(keys[2], 1), 0, NCLASS - 1).astype(jnp.int32),
        "filters": draw_filters(jax.random.fold_in(keys[6], 71), 0),
        "point_spread": draw_point_spread(jax.random.fold_in(keys[6], 71), 0),
        "spread_index": with_ends(jax.random.randint(keys[5], (BRICKS_X, BRICKS_Y), 0, NPSF), jax.random.fold_in(keys[5], 1), 0, NPSF - 1).astype(jnp.int32),
    }


HIGHEST = lax.Precision.HIGHEST

def advance(wavefield, velocity_class, filters_now, factor):
    padded = jnp.pad(wavefield, ((0, 0), (1, 1), (1, 1)))
    row_count = wavefield.shape[1]
    col_count = wavefield.shape[2]
    real_part = jnp.zeros((row_count, col_count), jnp.float32)
    imag_part = jnp.zeros((row_count, col_count), jnp.float32)
    for tap_index in range(9):
        row_shift = tap_index // 3
        col_shift = tap_index % 3
        near_real = padded[0, row_shift:row_shift + row_count, col_shift:col_shift + col_count]
        near_imag = padded[1, row_shift:row_shift + row_count, col_shift:col_shift + col_count]
        coef_real = filters_now[:, 0, tap_index][velocity_class]
        coef_imag = factor * filters_now[:, 1, tap_index][velocity_class]
        real_part = real_part + coef_real * near_real - coef_imag * near_imag
        imag_part = imag_part + coef_real * near_imag + coef_imag * near_real
    return jnp.stack([real_part, imag_part])

def lag_pick():
    depths = jnp.arange(STEPS, dtype=jnp.int32)
    spacing = jnp.abs(depths[:, None] - depths[None, :])
    return (spacing[None] == depths[:, None, None]).astype(jnp.float32)

def forward(model_cube, point_spread, spread_index):
    reach = PSF_SIDE // 2
    padded = jnp.pad(model_cube, ((0, 0), (reach, reach), (reach, reach)))
    picker = lag_pick()

    def one_brick(number):
        brick_row = number // BRICKS_Y
        brick_col = number % BRICKS_Y
        window = lax.dynamic_slice(padded, (jnp.zeros((), jnp.int32), brick_row * ROWS, brick_col * BCOLS), (STEPS, ROWS + 2 * reach, BCOLS + 2 * reach))
        kernel = jnp.einsum('lde,lab->edab', picker, point_spread[spread_index[brick_row, brick_col]], precision=HIGHEST)
        return lax.conv_general_dilated(window[None], kernel, (1, 1), 'VALID', precision=HIGHEST)[0]
    bricks = lax.map(one_brick, jnp.arange(BRICKS_X * BRICKS_Y, dtype=jnp.int32))
    bricks = bricks.reshape(BRICKS_X, BRICKS_Y, STEPS, ROWS, BCOLS)
    return bricks.transpose(2, 0, 3, 1, 4).reshape(STEPS, NX, NY)

def reference(receiver_field, source_field, velocity_class, filters, point_spread, spread_index):

    def one_frequency(summed, inputs):
        receiver, source, filters_now = inputs
        image_terms = []
        for depth_step in range(STEPS):
            receiver = advance(receiver, velocity_class, filters_now, 1.0)
            source = advance(source, velocity_class, filters_now, -1.0)
            image_terms.append(receiver[0] * source[0] + receiver[1] * source[1])
        return (summed + jnp.stack(image_terms, axis=1), None)
    start = jnp.zeros((NX, STEPS, NY), jnp.float32)
    summed, unused = lax.scan(one_frequency, start, (jnp.moveaxis(receiver_field, 1, 0), jnp.moveaxis(source_field, 1, 0), filters))
    migrated = summed * (1.0 / math.sqrt(NF))

    def operator(values):
        return forward(values, point_spread, spread_index)
    cell_count = STEPS * NX * NY
    residual = -jnp.transpose(migrated, (1, 0, 2))
    reflectivity = jnp.zeros_like(residual)
    energy = jnp.sum(residual * residual)
    for pass_index in range(PASSES):
        weight = 1.0 / jnp.sqrt(residual * residual + energy / cell_count)
        unused_out, pullback = jax.vjp(operator, reflectivity)
        descent = pullback(weight * residual)[0]
        image_of = operator(descent)
        step_length = jnp.sum(descent * descent) / jnp.sum(weight * image_of * image_of)
        reflectivity = reflectivity - step_length * descent
        residual = residual - step_length * image_of
        energy = jnp.sum(residual * residual)
    return (migrated, jnp.transpose(reflectivity, (1, 0, 2)), energy / cell_count)
```

```python
import functools
import math

import jax
import jax.numpy as jnp
from jax import lax
from jax.experimental import pallas as pl
from jax.experimental.pallas import tpu as pltpu
from jax.sharding import PartitionSpec as P

STEPS = 2
NCLASS = 8
PASSES = 2
MESH = pl.DeviceIdType.MESH


def kernel(
    groups,
    strips,
    near,
    spread_ref,
    filters_ref,
    receiver_ref,
    source_ref,
    class_ref,
    psf_ref,
    migrated_ref,
    reflect_ref,
    misfit_ref,
    rows_out,
    rows_in,
    class_in,
    fields,
    classes,
    shifted,
    coefs,
    terms,
    terms_in,
    own_table,
    table,
    rim_out,
    rim_in,
    rolled,
    spill,
    strip_spill,
    moved,
    sums_out,
    sums_in,
    send_sem,
    recv_sem,
    class_sem,
    rim_sem,
    sum_sem,
):
    freq = lax.axis_index("freq")
    strip = lax.axis_index("strip")
    total = groups * strips
    me = freq * strips + strip
    rows, cols = class_ref.shape
    share = migrated_ref.shape[2]
    side = psf_ref.shape[2]
    reach = side // 2
    wide = 2 * share
    reaches = [(dj, dk) for dj in range(-near, near + 1) for dk in (-1, 0, 1)]
    reaches.remove((0, 0))
    reaches.append((0, 0))
    place = {pair: at for at, pair in enumerate(reaches)}
    partners = len(reaches) - 1
    span = 2 * near + 1

    barrier = pltpu.get_barrier_semaphore()

    def greet(i, carry):
        other = lax.rem(me + i, total)
        pl.semaphore_signal(
            barrier,
            inc=1,
            device_id=(other // strips, lax.rem(other, strips)),
            device_id_type=MESH,
        )
        return carry

    lax.fori_loop(1, total, greet, 0)

    for field, ref in enumerate((receiver_ref, source_ref)):
        for part in range(2):
            at = 2 * (2 * field + part)
            rows_out[0, at : at + 2, :] = ref[part, 0, 0:2, :]
            rows_out[1, at : at + 2, :] = ref[part, 0, rows - 2 : rows, :]

    pl.semaphore_wait(barrier, total - 1)

    up = lax.rem(strip + strips - 1, strips)
    down = lax.rem(strip + 1, strips)
    copies = []
    for side_at, other in ((0, up), (1, down)):
        copies.append(
            pltpu.make_async_remote_copy(
                src_ref=rows_out.at[side_at],
                dst_ref=rows_in.at[side_at],
                send_sem=send_sem.at[side_at],
                recv_sem=recv_sem.at[side_at],
                device_id=(freq, other),
                device_id_type=MESH,
            )
        )
        copies.append(
            pltpu.make_async_remote_copy(
                src_ref=class_ref,
                dst_ref=class_in.at[side_at],
                send_sem=class_sem.at[side_at],
                recv_sem=class_sem.at[2 + side_at],
                device_id=(freq, other),
                device_id_type=MESH,
            )
        )
    for copy in copies:
        copy.start()

    lane = lax.broadcasted_iota(jnp.int32, (1, wide), 1)
    column = jnp.where(lane < wide - wide // 4, lane, lane - wide)

    def spread_of(row_step, col_step):
        row_at = jnp.clip(strip + row_step, 0, strips - 1)
        col_at = jnp.clip(freq + col_step, 0, groups - 1)
        chosen = spread_ref[row_at, col_at]
        both = psf_ref[chosen]
        return both[0] + both[1], both[0] - both[1]

    def fill(j, carry):
        left = spread_of(j - near, -1)
        middle = spread_of(j - near, 0)
        right = spread_of(j - near, 1)
        for st in range(2):
            for b in range(side):
                source_col = column - (b - reach)
                shape = (side, wide)
                k_left = jnp.broadcast_to(left[st][:, b : b + 1], shape)
                k_middle = jnp.broadcast_to(middle[st][:, b : b + 1], shape)
                k_right = jnp.broadcast_to(right[st][:, b : b + 1], shape)
                table[j * 2 + st, b, 0:side, :] = jnp.where(
                    source_col < 0, k_left, jnp.where(source_col >= share, k_right, k_middle)
                )
        return carry

    lax.fori_loop(0, span, fill, 0)
    own = spread_of(0, 0)
    for st in range(2):
        for b in range(side):
            own_table[st, b, 0:side, :] = jnp.broadcast_to(own[st][:, b : b + 1], (side, share))

    for field, ref in enumerate((receiver_ref, source_ref)):
        for part in range(2):
            fields[2 * field + part, rows : 2 * rows, :] = ref[part, 0]
    classes[rows : 2 * rows, :] = class_ref[...]
    for copy in copies:
        copy.wait()
    first = strip == 0
    last = strip == strips - 1
    for comp in range(4):
        above = rows_in[1, 2 * comp : 2 * comp + 2, :]
        below = rows_in[0, 2 * comp : 2 * comp + 2, :]
        fields[comp, rows - 2 : rows, :] = jnp.where(first, 0.0, above)
        fields[comp, 2 * rows : 2 * rows + 2, :] = jnp.where(last, 0.0, below)
    classes[rows - 1 : rows, :] = class_in[1, rows - 1 : rows, :]
    classes[2 * rows : 2 * rows + 1, :] = class_in[0, 0:1, :]

    levels = classes[rows - 1 : 3 * rows - 1, :]
    for part in range(2):
        for tap in range(9):
            value = jnp.full(levels.shape, filters_ref[0, 0, part, tap], jnp.float32)
            for level in range(1, NCLASS):
                value = jnp.where(levels == level, filters_ref[0, level, part, tap], value)
            coefs[part * 9 + tap] = value

    edge = lax.broadcasted_iota(jnp.int32, (1, cols), 1)

    def shift_all():
        for comp in range(4):
            base = fields[comp]
            shifted[comp, 0] = jnp.where(edge == 0, 0.0, pltpu.roll(base, 1, 1))
            shifted[comp, 1] = base
            shifted[comp, 2] = jnp.where(edge == cols - 1, 0.0, pltpu.roll(base, cols - 1, 1))

    def advance(field, start, count, skip):
        factor = 1.0 if field == 0 else -1.0
        real_part = jnp.zeros((count, cols), jnp.float32)
        imag_part = jnp.zeros((count, cols), jnp.float32)
        for tap in range(9):
            at = start + tap // 3 - 1
            near_real = shifted[2 * field, tap % 3, at : at + count, :]
            near_imag = shifted[2 * field + 1, tap % 3, at : at + count, :]
            coef_real = coefs[tap, skip : skip + count, :]
            coef_imag = factor * coefs[9 + tap, skip : skip + count, :]
            real_part = real_part + coef_real * near_real - coef_imag * near_imag
            imag_part = imag_part + coef_real * near_imag + coef_imag * near_real
        return real_part, imag_part

    shift_all()
    line = lax.broadcasted_iota(jnp.int32, (2 * rows, cols), 0)
    alive = (line < rows + 2) & ((line > 0) | (strip > 0)) & ((line < rows + 1) | (strip < strips - 1))
    ahead = advance(0, rows - 1, 2 * rows, 0) + advance(1, rows - 1, 2 * rows, 0)
    for comp in range(4):
        fields[comp, rows - 1 : 3 * rows - 1, :] = jnp.where(alive, ahead[comp], 0.0)
    shift_all()
    second = advance(0, rows, rows, 1) + advance(1, rows, rows, 1)
    firsts = [fields[comp, rows : 2 * rows, :] for comp in range(4)]
    for depth, f in enumerate((firsts, second)):
        image = f[0] * f[2] + f[1] * f[3]
        for g in range(groups):
            terms[g, depth] = image[:, g * share : (g + 1) * share]

    def send_terms(i, carry):
        other = lax.rem(freq + i, groups)
        pltpu.make_async_remote_copy(
            src_ref=terms.at[other],
            dst_ref=terms_in.at[i - 1],
            send_sem=send_sem.at[2],
            recv_sem=recv_sem.at[2],
            device_id=(other, strip),
            device_id_type=MESH,
        ).start()
        return carry

    def wait_all(buffer, sem):
        pltpu.make_async_copy(buffer, buffer, sem).wait()

    lax.fori_loop(1, groups, send_terms, 0)
    wait_all(terms_in, recv_sem.at[2])
    scaling = 1.0 / math.sqrt(groups)
    migrated = terms[freq]
    for i in range(groups - 1):
        migrated = migrated + terms_in[i]
    migrated = migrated * scaling
    for depth in range(STEPS):
        migrated_ref[:, depth, :] = migrated[depth]

    def send_rim(value, turn):
        rim_out[turn] = value
        rim_in[turn, partners] = value
        for dj, dk in reaches[:-1]:
            pltpu.make_async_remote_copy(
                src_ref=rim_out.at[turn],
                dst_ref=rim_in.at[turn, place[(-dj, -dk)]],
                send_sem=rim_sem.at[2 * turn],
                recv_sem=rim_sem.at[2 * turn + 1],
                device_id=(
                    lax.rem(freq + dk + groups, groups),
                    lax.rem(strip + dj + near * strips, strips),
                ),
                device_id_type=MESH,
            ).start()

    quarter = share // 4
    slim = lax.broadcasted_iota(jnp.int32, (1, share), 1)

    def send_sums(parts, turn):
        row = jnp.zeros((1, share), jnp.float32)
        for at, part in enumerate(parts):
            lanes = jnp.sum(part, axis=0, keepdims=True)
            lanes = lanes + pltpu.roll(lanes, share // 2, 1)
            lanes = lanes + pltpu.roll(lanes, quarter, 1)
            row = jnp.where((slim >= at * quarter) & (slim < (at + 1) * quarter), lanes, row)
        sums_out[turn] = row

        def send(i, carry):
            other = lax.rem(me + i, total)
            pltpu.make_async_remote_copy(
                src_ref=sums_out.at[turn],
                dst_ref=sums_in.at[turn, i - 1],
                send_sem=sum_sem.at[2 * turn],
                recv_sem=sum_sem.at[2 * turn + 1],
                device_id=(other // strips, lax.rem(other, strips)),
                device_id_type=MESH,
            ).start()
            return carry

        lax.fori_loop(1, total, send, 0)
        return row

    def take_sums(row, turn, count):
        wait_all(sums_in.at[turn], sum_sem.at[2 * turn + 1])
        row = row + jnp.sum(sums_in[turn], axis=0)
        return [
            jnp.sum(
                jnp.where((slim >= at * quarter) & (slim < (at + 1) * quarter), row, 0.0),
                axis=1,
                keepdims=True,
            )
            for at in range(count)
        ]

    def rim_values(turn):
        found = []
        for dj in range(-near, near + 1):
            ok = (strip + dj >= 0) & (strip + dj < strips)
            pair = []
            for depth in range(STEPS):
                middle = jnp.where(ok, rim_in[turn, place[(dj, 0)], depth], 0.0)
                right = jnp.where(ok & (freq < groups - 1), rim_in[turn, place[(dj, 1)], depth], 0.0)
                left = jnp.where(ok & (freq > 0), rim_in[turn, place[(dj, -1)], depth], 0.0)
                outer = jnp.where(
                    slim < 2 * reach, right, jnp.where(slim >= share - 2 * reach, left, 0.0)
                )
                pair.append(jnp.concatenate([middle, outer], axis=1))
            found.append(pair)
        return found

    tall = 3 * rows

    def descend(weighted):
        for j in range(span):
            for st in range(2):
                both = weighted[j][0] + weighted[j][1] if st == 0 else weighted[j][0] - weighted[j][1]
                for b in range(side):
                    rolled[2 * j + st, b] = pltpu.roll(both, (b - reach) % wide, 1)
        spill[...] = jnp.zeros_like(spill)

        def one(index, carry):
            j = index // 2
            st = lax.rem(index, 2)
            strip_spill[...] = jnp.zeros_like(strip_spill)
            for low in (0, 5, 10):
                high = min(low + 5, side)
                totals = [jnp.zeros((rows, wide), jnp.float32) for a in range(low, high)]
                for b in range(side):
                    data = rolled[index, b]
                    for a in range(low, high):
                        totals[a - low] = totals[a - low] + table[index, b, a : a + 1, :] * data
                for a in range(low, high):
                    strip_spill[a : a + rows, :] += totals[a - low]
            at = pl.ds(pl.multiple_of(rows * j, rows), tall)
            spill[st, at, :] += strip_spill[...]
            return carry

        lax.fori_loop(0, 2 * span, one, 0)
        depth_line = lax.broadcasted_iota(jnp.int32, (tall, wide), 0) - reach + strip * rows
        at_col = column + freq * share
        ok = (
            (depth_line >= 0)
            & (depth_line < strips * rows)
            & (at_col >= 0)
            & (at_col < groups * share)
        )
        base = near * rows
        values = [jnp.where(ok, spill[st, base : base + tall, :], 0.0) for st in range(2)]
        for st in range(2):
            spill[st, base : base + tall, :] = values[st]
        mine = [spill[st, base + reach : base + reach + rows, 0:share] for st in range(2)]
        descent = [0.5 * (mine[0] + mine[1]), 0.5 * (mine[0] - mine[1])]
        image = [jnp.zeros((rows, share), jnp.float32) for st in range(2)]
        for st in range(2):
            for b in range(side):
                moved[st, b] = pltpu.roll(values[st], (reach - b) % wide, 1)[:, 0:share]
            for b in range(side):
                for a in range(side):
                    image[st] = image[st] + own_table[st, b, a : a + 1, :] * moved[st, b, a : a + rows, :]
        image_of = [0.5 * (image[0] + image[1]), 0.5 * (image[0] - image[1])]
        return descent, image_of

    cells = float(STEPS * rows * strips * cols)
    send_rim(-migrated, 0)
    row = send_sums([migrated[0] * migrated[0] + migrated[1] * migrated[1]], 0)
    wait_all(rim_in.at[0, 0:partners], rim_sem.at[1])
    residual = rim_values(0)
    (energy,) = take_sums(row, 0, 1)
    reflect = [jnp.zeros((rows, share), jnp.float32) for depth in range(STEPS)]
    for turn in range(1, PASSES + 1):
        weights = [
            [1.0 / jnp.sqrt(r * r + energy / cells) for r in pair] for pair in residual
        ]
        weighted = [[w * r for w, r in zip(ws, rs)] for ws, rs in zip(weights, residual)]
        descent, image_of = descend(weighted)
        if turn < PASSES:
            send_rim(jnp.stack(image_of), turn)
        parts = [jnp.zeros((rows, share), jnp.float32) for q in range(4)]
        for depth in range(STEPS):
            v = image_of[depth]
            r = residual[near][depth][:, 0:share]
            w = weights[near][depth][:, 0:share]
            parts[0] = parts[0] + descent[depth] * descent[depth]
            parts[1] = parts[1] + w * v * v
            parts[2] = parts[2] + r * v
            parts[3] = parts[3] + v * v
        row = send_sums(parts, turn)
        if turn < PASSES:
            wait_all(rim_in.at[turn, 0:partners], rim_sem.at[2 * turn + 1])
            images = rim_values(turn)
        grad_square, curvature, cross_term, power_term = take_sums(row, turn, 4)
        step_length = grad_square / curvature
        energy = energy - 2.0 * step_length * cross_term + step_length * step_length * power_term
        reflect = [x - step_length * d for x, d in zip(reflect, descent)]
        if turn < PASSES:
            residual = [
                [r - step_length * v for r, v in zip(rs, vs)] for rs, vs in zip(residual, images)
            ]
    for depth in range(STEPS):
        reflect_ref[:, depth, :] = reflect[depth]
    misfit_ref[...] = energy / cells

    wait_all(terms_in, send_sem.at[2])
    for turn in range(PASSES):
        wait_all(rim_in.at[turn, 0:partners], rim_sem.at[2 * turn])
    for turn in range(PASSES + 1):
        wait_all(sums_in.at[turn], sum_sem.at[2 * turn])


def local(receiver_field, source_field, velocity_class, filters, point_spread, spread_index):
    groups = lax.axis_size("freq")
    strips = lax.axis_size("strip")
    rows, cols = velocity_class.shape
    share = cols // groups
    side = point_spread.shape[2]
    reach = side // 2
    near = -(-2 * reach // rows)
    partners = 3 * (2 * near + 1) - 1
    total = groups * strips
    wide = 2 * share
    vmem = pl.BlockSpec(memory_space=pltpu.VMEM)
    smem = pl.BlockSpec(memory_space=pltpu.SMEM)
    f32 = jnp.float32
    dma = pltpu.SemaphoreType.DMA
    deep = -(-(rows * (2 * near + 1) + side) // 8) * 8
    migrated, reflectivity, misfit = pl.pallas_call(
        functools.partial(kernel, groups, strips, near),
        out_shape=(
            jax.ShapeDtypeStruct((rows, STEPS, share), f32),
            jax.ShapeDtypeStruct((rows, STEPS, share), f32),
            jax.ShapeDtypeStruct((1, 1), f32),
        ),
        in_specs=[smem, smem, vmem, vmem, vmem, vmem],
        out_specs=(vmem, vmem, vmem),
        scratch_shapes=[
            pltpu.VMEM((2, 8, cols), f32),
            pltpu.VMEM((2, 8, cols), f32),
            pltpu.VMEM((2, rows, cols), jnp.int32),
            pltpu.VMEM((4, 3 * rows, cols), f32),
            pltpu.VMEM((3 * rows, cols), jnp.int32),
            pltpu.VMEM((4, 3, 3 * rows, cols), f32),
            pltpu.VMEM((18, 2 * rows, cols), f32),
            pltpu.VMEM((groups, STEPS, rows, share), f32),
            pltpu.VMEM((groups - 1, STEPS, rows, share), f32),
            pltpu.VMEM((2, side, 16, share), f32),
            pltpu.VMEM((2 * (2 * near + 1), side, 16, wide), f32),
            pltpu.VMEM((PASSES, STEPS, rows, share), f32),
            pltpu.VMEM((PASSES, partners + 1, STEPS, rows, share), f32),
            pltpu.VMEM((2 * (2 * near + 1), side, rows, wide), f32),
            pltpu.VMEM((2, deep, wide), f32),
            pltpu.VMEM((3 * rows, wide), f32),
            pltpu.VMEM((2, side, 3 * rows, share), f32),
            pltpu.VMEM((PASSES + 1, 1, share), f32),
            pltpu.VMEM((PASSES + 1, total - 1, 1, share), f32),
            dma((3,)),
            dma((3,)),
            dma((4,)),
            dma((2 * PASSES,)),
            dma((2 * (PASSES + 1),)),
        ],
        compiler_params=pltpu.CompilerParams(collective_id=0, has_side_effects=True),
    )(spread_index, filters, receiver_field, source_field, velocity_class, point_spread)
    return migrated, reflectivity, misfit[0, 0]


def solution(mesh):
    return jax.shard_map(
        local,
        mesh=mesh,
        in_specs=(
            P(None, "freq", "strip", None),
            P(None, "freq", "strip", None),
            P("strip", None),
            P("freq", None, None, None),
            P(),
            P(),
        ),
        out_specs=(P("strip", None, "freq"), P("strip", None, "freq"), P()),
        check_vma=False,
    )
```

```python
import functools
import math

import jax
import jax.numpy as jnp
from jax import lax
from jax.experimental import pallas as pl
from jax.experimental.pallas import tpu as pltpu
from jax.sharding import PartitionSpec as P

STEPS = 2
NCLASS = 8
PASSES = 2
MESH = pl.DeviceIdType.MESH


def kernel(
    groups,
    strips,
    near,
    spread_ref,
    filters_ref,
    receiver_ref,
    source_ref,
    class_ref,
    psf_ref,
    migrated_ref,
    reflect_ref,
    misfit_ref,
    rows_out,
    rows_in,
    class_out,
    class_in,
    fields,
    classes,
    shifted,
    coefs,
    terms,
    terms_in,
    by_index,
    own_table,
    table,
    rim_out,
    rim_in,
    rolled,
    spill,
    strip_spill,
    moved,
    sums_out,
    sums_in,
    send_sem,
    recv_sem,
    class_sem,
    rim_sem,
    sum_sem,
):
    freq = lax.axis_index("freq")
    strip = lax.axis_index("strip")
    total = groups * strips
    me = freq * strips + strip
    rows, cols = class_ref.shape
    share = migrated_ref.shape[2]
    side = psf_ref.shape[0]
    count = psf_ref.shape[3]
    reach = side // 2
    wide = 2 * share
    reaches = [(dj, dk) for dj in range(-near, near + 1) for dk in (-1, 0, 1)]
    reaches.remove((0, 0))
    reaches.append((0, 0))
    place = {pair: at for at, pair in enumerate(reaches)}
    partners = len(reaches) - 1
    span = 2 * near + 1

    barrier = pltpu.get_barrier_semaphore()

    for i in range(1, groups):
        pl.semaphore_signal(
            barrier,
            inc=1,
            device_id=(lax.rem(freq + i, groups), strip),
            device_id_type=MESH,
        )
    for i in range(1, strips):
        pl.semaphore_signal(
            barrier,
            inc=1,
            device_id=(freq, lax.rem(strip + i, strips)),
            device_id_type=MESH,
        )

    for field, ref in enumerate((receiver_ref, source_ref)):
        for part in range(2):
            at = 2 * (2 * field + part)
            rows_out[0, at : at + 2, :] = ref[part, 0, 0:2, :]
            rows_out[1, at : at + 2, :] = ref[part, 0, rows - 2 : rows, :]

    class_out[0] = class_ref[0:1, :]
    class_out[1] = class_ref[rows - 1 : rows, :]

    lane = lax.broadcasted_iota(jnp.int32, (1, wide), 1)
    column = jnp.where(lane < wide - wide // 4, lane, lane - wide)

    def spread_of(row_step, col_step):
        row_at = jnp.clip(strip + row_step, 0, strips - 1)
        col_at = jnp.clip(freq + col_step, 0, groups - 1)
        return spread_ref[col_at, row_at]

    for a in range(side):
        for b in range(side):
            pair = psf_ref[a, b]
            by_index[0, b, a : a + 1, 0:count] = pair[0:1] + pair[1:2]
            by_index[1, b, a : a + 1, 0:count] = pair[0:1] - pair[1:2]
    pick = lax.broadcasted_iota(jnp.int32, (16, share), 1)

    def taps_of(st, b, chosen):
        kept = jnp.where(pick == chosen, by_index[st, b], 0.0)
        return jnp.sum(kept, axis=1, keepdims=True)

    def fill(j, carry):
        left = spread_of(j - near, -1)
        middle = spread_of(j - near, 0)
        right = spread_of(j - near, 1)
        for st in range(2):
            for b in range(side):
                source_col = column - (b - reach)
                shape = (16, wide)
                k_left = jnp.broadcast_to(taps_of(st, b, left), shape)
                k_middle = jnp.broadcast_to(taps_of(st, b, middle), shape)
                k_right = jnp.broadcast_to(taps_of(st, b, right), shape)
                table[j * 2 + st, b] = jnp.where(
                    source_col < 0, k_left, jnp.where(source_col >= share, k_right, k_middle)
                )
        return carry

    lax.fori_loop(0, span, fill, 0)
    own = spread_of(0, 0)
    for st in range(2):
        for b in range(side):
            own_table[st, b] = jnp.broadcast_to(taps_of(st, b, own), (16, share))

    pl.semaphore_wait(barrier, groups + strips - 2)

    up = lax.rem(strip + strips - 1, strips)
    down = lax.rem(strip + 1, strips)
    copies = []
    for side_at, other in ((0, up), (1, down)):
        copies.append(
            pltpu.make_async_remote_copy(
                src_ref=rows_out.at[side_at],
                dst_ref=rows_in.at[side_at],
                send_sem=send_sem.at[side_at],
                recv_sem=recv_sem.at[side_at],
                device_id=(freq, other),
                device_id_type=MESH,
            )
        )
        copies.append(
            pltpu.make_async_remote_copy(
                src_ref=class_out.at[side_at],
                dst_ref=class_in.at[side_at],
                send_sem=class_sem.at[side_at],
                recv_sem=class_sem.at[2 + side_at],
                device_id=(freq, other),
                device_id_type=MESH,
            )
        )
    for copy in copies:
        copy.start()

    for field, ref in enumerate((receiver_ref, source_ref)):
        for part in range(2):
            fields[2 * field + part, rows : 2 * rows, :] = ref[part, 0]
    classes[rows : 2 * rows, :] = class_ref[...]
    for copy in copies:
        copy.wait()
    first = strip == 0
    last = strip == strips - 1
    for comp in range(4):
        above = rows_in[1, 2 * comp : 2 * comp + 2, :]
        below = rows_in[0, 2 * comp : 2 * comp + 2, :]
        fields[comp, rows - 2 : rows, :] = jnp.where(first, 0.0, above)
        fields[comp, 2 * rows : 2 * rows + 2, :] = jnp.where(last, 0.0, below)
    classes[rows - 1 : rows, :] = class_in[1]
    classes[2 * rows : 2 * rows + 1, :] = class_in[0]

    levels = classes[rows - 1 : 3 * rows - 1, :]
    for part in range(2):
        for tap in range(9):
            value = jnp.full(levels.shape, filters_ref[0, 0, part, tap], jnp.float32)
            for level in range(1, NCLASS):
                value = jnp.where(levels == level, filters_ref[0, level, part, tap], value)
            coefs[part * 9 + tap] = value

    edge = lax.broadcasted_iota(jnp.int32, (1, cols), 1)

    def shift_all():
        for comp in range(4):
            base = fields[comp]
            shifted[comp, 0] = jnp.where(edge == 0, 0.0, pltpu.roll(base, 1, 1))
            shifted[comp, 1] = base
            shifted[comp, 2] = jnp.where(edge == cols - 1, 0.0, pltpu.roll(base, cols - 1, 1))

    def advance(field, start, count, skip):
        factor = 1.0 if field == 0 else -1.0
        real_part = jnp.zeros((count, cols), jnp.float32)
        imag_part = jnp.zeros((count, cols), jnp.float32)
        for tap in range(9):
            at = start + tap // 3 - 1
            near_real = shifted[2 * field, tap % 3, at : at + count, :]
            near_imag = shifted[2 * field + 1, tap % 3, at : at + count, :]
            coef_real = coefs[tap, skip : skip + count, :]
            coef_imag = factor * coefs[9 + tap, skip : skip + count, :]
            real_part = real_part + coef_real * near_real - coef_imag * near_imag
            imag_part = imag_part + coef_real * near_imag + coef_imag * near_real
        return real_part, imag_part

    shift_all()
    line = lax.broadcasted_iota(jnp.int32, (2 * rows, cols), 0)
    alive = (line < rows + 2) & ((line > 0) | (strip > 0)) & ((line < rows + 1) | (strip < strips - 1))
    ahead = advance(0, rows - 1, 2 * rows, 0) + advance(1, rows - 1, 2 * rows, 0)
    for comp in range(4):
        fields[comp, rows - 1 : 3 * rows - 1, :] = jnp.where(alive, ahead[comp], 0.0)
    shift_all()
    second = advance(0, rows, rows, 1) + advance(1, rows, rows, 1)
    firsts = [fields[comp, rows : 2 * rows, :] for comp in range(4)]
    for depth, f in enumerate((firsts, second)):
        image = f[0] * f[2] + f[1] * f[3]
        for g in range(groups):
            terms[g, depth] = image[:, g * share : (g + 1) * share]

    def send_terms(i, carry):
        other = lax.rem(freq + i, groups)
        pltpu.make_async_remote_copy(
            src_ref=terms.at[other],
            dst_ref=terms_in.at[i - 1],
            send_sem=send_sem.at[2],
            recv_sem=recv_sem.at[2],
            device_id=(other, strip),
            device_id_type=MESH,
        ).start()
        return carry

    def wait_all(buffer, sem):
        pltpu.make_async_copy(buffer, buffer, sem).wait()

    lax.fori_loop(1, groups, send_terms, 0)
    wait_all(terms_in, recv_sem.at[2])
    scaling = 1.0 / math.sqrt(groups)
    migrated = terms[freq]
    for i in range(groups - 1):
        migrated = migrated + terms_in[i]
    migrated = migrated * scaling
    for depth in range(STEPS):
        migrated_ref[:, depth, :] = migrated[depth]

    def send_rim(value, turn):
        rim_out[turn] = value
        rim_in[turn, partners] = value
        for dj, dk in reaches[:-1]:
            pltpu.make_async_remote_copy(
                src_ref=rim_out.at[turn],
                dst_ref=rim_in.at[turn, place[(-dj, -dk)]],
                send_sem=rim_sem.at[2 * turn],
                recv_sem=rim_sem.at[2 * turn + 1],
                device_id=(
                    lax.rem(freq + dk + groups, groups),
                    lax.rem(strip + dj + near * strips, strips),
                ),
                device_id_type=MESH,
            ).start()

    quarter = share // 4
    slim = lax.broadcasted_iota(jnp.int32, (1, share), 1)

    def send_sums(parts, turn):
        row = jnp.zeros((1, share), jnp.float32)
        for at, part in enumerate(parts):
            lanes = jnp.sum(part, axis=0, keepdims=True)
            lanes = lanes + pltpu.roll(lanes, share // 2, 1)
            lanes = lanes + pltpu.roll(lanes, quarter, 1)
            row = jnp.where((slim >= at * quarter) & (slim < (at + 1) * quarter), lanes, row)
        sums_out[turn] = row

        def send(i, carry):
            other = lax.rem(me + i, total)
            pltpu.make_async_remote_copy(
                src_ref=sums_out.at[turn],
                dst_ref=sums_in.at[turn, i - 1],
                send_sem=sum_sem.at[2 * turn],
                recv_sem=sum_sem.at[2 * turn + 1],
                device_id=(other // strips, lax.rem(other, strips)),
                device_id_type=MESH,
            ).start()
            return carry

        lax.fori_loop(1, total, send, 0)
        return row

    def take_sums(row, turn, count):
        wait_all(sums_in.at[turn], sum_sem.at[2 * turn + 1])
        row = row + jnp.sum(sums_in[turn], axis=0)
        return [
            jnp.sum(
                jnp.where((slim >= at * quarter) & (slim < (at + 1) * quarter), row, 0.0),
                axis=1,
                keepdims=True,
            )
            for at in range(count)
        ]

    def rim_values(turn):
        found = []
        for dj in range(-near, near + 1):
            ok = (strip + dj >= 0) & (strip + dj < strips)
            pair = []
            for depth in range(STEPS):
                middle = jnp.where(ok, rim_in[turn, place[(dj, 0)], depth], 0.0)
                right = jnp.where(ok & (freq < groups - 1), rim_in[turn, place[(dj, 1)], depth], 0.0)
                left = jnp.where(ok & (freq > 0), rim_in[turn, place[(dj, -1)], depth], 0.0)
                outer = jnp.where(
                    slim < 2 * reach, right, jnp.where(slim >= share - 2 * reach, left, 0.0)
                )
                pair.append(jnp.concatenate([middle, outer], axis=1))
            found.append(pair)
        return found

    tall = 3 * rows

    def descend(weighted):
        for j in range(span):
            for st in range(2):
                both = weighted[j][0] + weighted[j][1] if st == 0 else weighted[j][0] - weighted[j][1]
                for b in range(side):
                    rolled[2 * j + st, b] = pltpu.roll(both, (b - reach) % wide, 1)
        spill[...] = jnp.zeros_like(spill)

        def one(index, carry):
            j = index // 2
            st = lax.rem(index, 2)
            strip_spill[...] = jnp.zeros_like(strip_spill)
            for low in (0, 5, 10):
                high = min(low + 5, side)
                totals = [jnp.zeros((rows, wide), jnp.float32) for a in range(low, high)]
                for b in range(side):
                    data = rolled[index, b]
                    for a in range(low, high):
                        totals[a - low] = totals[a - low] + table[index, b, a : a + 1, :] * data
                for a in range(low, high):
                    strip_spill[a : a + rows, :] += totals[a - low]
            at = pl.ds(pl.multiple_of(rows * j, rows), tall)
            spill[st, at, :] += strip_spill[...]
            return carry

        lax.fori_loop(0, 2 * span, one, 0)
        depth_line = lax.broadcasted_iota(jnp.int32, (tall, wide), 0) - reach + strip * rows
        at_col = column + freq * share
        ok = (
            (depth_line >= 0)
            & (depth_line < strips * rows)
            & (at_col >= 0)
            & (at_col < groups * share)
        )
        base = near * rows
        values = [jnp.where(ok, spill[st, base : base + tall, :], 0.0) for st in range(2)]
        for st in range(2):
            spill[st, base : base + tall, :] = values[st]
        mine = [spill[st, base + reach : base + reach + rows, 0:share] for st in range(2)]
        descent = [0.5 * (mine[0] + mine[1]), 0.5 * (mine[0] - mine[1])]
        image = [jnp.zeros((rows, share), jnp.float32) for st in range(2)]
        for st in range(2):
            for b in range(side):
                moved[st, b] = pltpu.roll(values[st], (reach - b) % wide, 1)[:, 0:share]
            for b in range(side):
                for a in range(side):
                    image[st] = image[st] + own_table[st, b, a : a + 1, :] * moved[st, b, a : a + rows, :]
        image_of = [0.5 * (image[0] + image[1]), 0.5 * (image[0] - image[1])]
        return descent, image_of

    cells = float(STEPS * rows * strips * cols)
    row = send_sums([migrated[0] * migrated[0] + migrated[1] * migrated[1]], 0)
    send_rim(-migrated, 0)
    wait_all(rim_in.at[0, 0:partners], rim_sem.at[1])
    residual = rim_values(0)
    (energy,) = take_sums(row, 0, 1)
    reflect = [jnp.zeros((rows, share), jnp.float32) for depth in range(STEPS)]
    for turn in range(1, PASSES + 1):
        weights = [
            [1.0 / jnp.sqrt(r * r + energy / cells) for r in pair] for pair in residual
        ]
        weighted = [[w * r for w, r in zip(ws, rs)] for ws, rs in zip(weights, residual)]
        descent, image_of = descend(weighted)
        parts = [jnp.zeros((rows, share), jnp.float32) for q in range(4)]
        for depth in range(STEPS):
            v = image_of[depth]
            r = residual[near][depth][:, 0:share]
            w = weights[near][depth][:, 0:share]
            parts[0] = parts[0] + descent[depth] * descent[depth]
            parts[1] = parts[1] + w * v * v
            parts[2] = parts[2] + r * v
            parts[3] = parts[3] + v * v
        row = send_sums(parts, turn)
        if turn < PASSES:
            send_rim(jnp.stack(image_of), turn)
            wait_all(rim_in.at[turn, 0:partners], rim_sem.at[2 * turn + 1])
            images = rim_values(turn)
        grad_square, curvature, cross_term, power_term = take_sums(row, turn, 4)
        step_length = grad_square / curvature
        energy = energy - 2.0 * step_length * cross_term + step_length * step_length * power_term
        reflect = [x - step_length * d for x, d in zip(reflect, descent)]
        if turn < PASSES:
            residual = [
                [r - step_length * v for r, v in zip(rs, vs)] for rs, vs in zip(residual, images)
            ]
    for depth in range(STEPS):
        reflect_ref[:, depth, :] = reflect[depth]
    misfit_ref[...] = energy / cells

    wait_all(terms_in, send_sem.at[2])
    for turn in range(PASSES):
        wait_all(rim_in.at[turn, 0:partners], rim_sem.at[2 * turn])
    for turn in range(PASSES + 1):
        wait_all(sums_in.at[turn], sum_sem.at[2 * turn])


def local(receiver_field, source_field, velocity_class, filters, point_spread, spread_index):
    groups = lax.axis_size("freq")
    strips = lax.axis_size("strip")
    rows, cols = velocity_class.shape
    share = cols // groups
    side = point_spread.shape[2]
    reach = side // 2
    near = -(-2 * reach // rows)
    partners = 3 * (2 * near + 1) - 1
    total = groups * strips
    wide = 2 * share
    vmem = pl.BlockSpec(memory_space=pltpu.VMEM)
    smem = pl.BlockSpec(memory_space=pltpu.SMEM)
    f32 = jnp.float32
    dma = pltpu.SemaphoreType.DMA
    deep = -(-(rows * (2 * near + 1) + side) // 8) * 8
    migrated, reflectivity, misfit = pl.pallas_call(
        functools.partial(kernel, groups, strips, near),
        out_shape=(
            jax.ShapeDtypeStruct((rows, STEPS, share), f32),
            jax.ShapeDtypeStruct((rows, STEPS, share), f32),
            jax.ShapeDtypeStruct((1, 1), f32),
        ),
        in_specs=[smem, smem, vmem, vmem, vmem, vmem],
        out_specs=(vmem, vmem, vmem),
        scratch_shapes=[
            pltpu.VMEM((2, 8, cols), f32),
            pltpu.VMEM((2, 8, cols), f32),
            pltpu.VMEM((2, 1, cols), jnp.int32),
            pltpu.VMEM((2, 1, cols), jnp.int32),
            pltpu.VMEM((4, 3 * rows, cols), f32),
            pltpu.VMEM((3 * rows, cols), jnp.int32),
            pltpu.VMEM((4, 3, 3 * rows, cols), f32),
            pltpu.VMEM((18, 2 * rows, cols), f32),
            pltpu.VMEM((groups, STEPS, rows, share), f32),
            pltpu.VMEM((groups - 1, STEPS, rows, share), f32),
            pltpu.VMEM((2, side, 16, share), f32),
            pltpu.VMEM((2, side, 16, share), f32),
            pltpu.VMEM((2 * (2 * near + 1), side, 16, wide), f32),
            pltpu.VMEM((PASSES, STEPS, rows, share), f32),
            pltpu.VMEM((PASSES, partners + 1, STEPS, rows, share), f32),
            pltpu.VMEM((2 * (2 * near + 1), side, rows, wide), f32),
            pltpu.VMEM((2, deep, wide), f32),
            pltpu.VMEM((3 * rows, wide), f32),
            pltpu.VMEM((2, side, 3 * rows, share), f32),
            pltpu.VMEM((PASSES + 1, 1, share), f32),
            pltpu.VMEM((PASSES + 1, total - 1, 1, share), f32),
            dma((3,)),
            dma((3,)),
            dma((4,)),
            dma((2 * PASSES,)),
            dma((2 * (PASSES + 1),)),
        ],
        compiler_params=pltpu.CompilerParams(collective_id=0, has_side_effects=True),
    )(
        spread_index.T,
        filters,
        receiver_field,
        source_field,
        velocity_class,
        jnp.transpose(point_spread, (2, 3, 1, 0)),
    )
    return migrated, reflectivity, misfit[0, 0]


def solution(mesh):
    return jax.shard_map(
        local,
        mesh=mesh,
        in_specs=(
            P(None, "freq", "strip", None),
            P(None, "freq", "strip", None),
            P("strip", None),
            P("freq", None, None, None),
            P(),
            P(),
        ),
        out_specs=(P("strip", None, "freq"), P("strip", None, "freq"), P()),
        check_vma=False,
    )
```

```python
import functools
import math

import jax
import jax.numpy as jnp
from jax import lax
from jax.experimental import pallas as pl
from jax.experimental.pallas import tpu as pltpu
from jax.sharding import PartitionSpec as P

STEPS = 2
NCLASS = 8
PASSES = 2
MESH = pl.DeviceIdType.MESH


def kernel(
    groups,
    strips,
    near,
    spread_ref,
    filters_ref,
    receiver_ref,
    source_ref,
    class_ref,
    psf_ref,
    migrated_ref,
    reflect_ref,
    misfit_ref,
    rows_out,
    rows_in,
    class_out,
    class_in,
    fields,
    classes,
    shifted,
    coefs,
    terms,
    terms_in,
    by_index,
    own_table,
    table,
    rim_out,
    rim_in,
    edge_out,
    edge_in,
    rolled,
    spill,
    moved,
    sums_out,
    sums_in,
    send_sem,
    recv_sem,
    class_sem,
    rim_sem,
    edge_sem,
    sum_sem,
):
    freq = lax.axis_index("freq")
    strip = lax.axis_index("strip")
    total = groups * strips
    me = freq * strips + strip
    rows, cols = class_ref.shape
    share = migrated_ref.shape[2]
    side = psf_ref.shape[0]
    count = psf_ref.shape[3]
    reach = side // 2
    wide = 2 * share
    reaches = [(dj, dk) for dj in range(-near, near + 1) for dk in (-1, 0, 1)]
    reaches.remove((0, 0))
    reaches.append((0, 0))
    span = 2 * near + 1
    rim_place = {dj: at for at, dj in enumerate([d for d in range(-near, near + 1) if d] + [0])}
    edge_place = {pair: at for at, pair in enumerate([p for p in reaches if p[1]])}

    barrier = pltpu.get_barrier_semaphore()

    for i in range(1, groups):
        pl.semaphore_signal(
            barrier,
            inc=1,
            device_id=(lax.rem(freq + i, groups), strip),
            device_id_type=MESH,
        )
    for i in range(1, strips):
        pl.semaphore_signal(
            barrier,
            inc=1,
            device_id=(freq, lax.rem(strip + i, strips)),
            device_id_type=MESH,
        )

    for field, ref in enumerate((receiver_ref, source_ref)):
        for part in range(2):
            at = 2 * (2 * field + part)
            rows_out[0, at : at + 2, :] = ref[part, 0, 0:2, :]
            rows_out[1, at : at + 2, :] = ref[part, 0, rows - 2 : rows, :]

    class_out[0] = class_ref[0:1, :]
    class_out[1] = class_ref[rows - 1 : rows, :]

    lane = lax.broadcasted_iota(jnp.int32, (1, wide), 1)
    column = jnp.where(lane < wide - wide // 4, lane, lane - wide)

    def spread_of(row_step, col_step):
        row_at = jnp.clip(strip + row_step, 0, strips - 1)
        col_at = jnp.clip(freq + col_step, 0, groups - 1)
        return spread_ref[col_at, row_at]

    for a in range(side):
        for b in range(side):
            pair = psf_ref[a, b]
            by_index[0, b, a : a + 1, 0:count] = pair[0:1] + pair[1:2]
            by_index[1, b, a : a + 1, 0:count] = pair[0:1] - pair[1:2]
    pick = lax.broadcasted_iota(jnp.int32, (16, share), 1)

    def taps_of(st, b, chosen):
        kept = jnp.where(pick == chosen, by_index[st, b], 0.0)
        return jnp.sum(kept, axis=1, keepdims=True)

    def fill(j, carry):
        left = spread_of(j - near, -1)
        middle = spread_of(j - near, 0)
        right = spread_of(j - near, 1)
        for st in range(2):
            for b in range(side):
                source_col = column - (b - reach)
                shape = (16, wide)
                k_left = jnp.broadcast_to(taps_of(st, b, left), shape)
                k_middle = jnp.broadcast_to(taps_of(st, b, middle), shape)
                k_right = jnp.broadcast_to(taps_of(st, b, right), shape)
                table[j * 2 + st, b] = jnp.where(
                    source_col < 0, k_left, jnp.where(source_col >= share, k_right, k_middle)
                )
        return carry

    lax.fori_loop(0, span, fill, 0)
    own = spread_of(0, 0)
    for st in range(2):
        for b in range(side):
            own_table[st, b] = jnp.broadcast_to(taps_of(st, b, own), (16, share))

    pl.semaphore_wait(barrier, groups + strips - 2)

    up = lax.rem(strip + strips - 1, strips)
    down = lax.rem(strip + 1, strips)
    copies = []
    for side_at, other in ((0, up), (1, down)):
        copies.append(
            pltpu.make_async_remote_copy(
                src_ref=rows_out.at[side_at],
                dst_ref=rows_in.at[side_at],
                send_sem=send_sem.at[side_at],
                recv_sem=recv_sem.at[side_at],
                device_id=(freq, other),
                device_id_type=MESH,
            )
        )
        copies.append(
            pltpu.make_async_remote_copy(
                src_ref=class_out.at[side_at],
                dst_ref=class_in.at[side_at],
                send_sem=class_sem.at[side_at],
                recv_sem=class_sem.at[2 + side_at],
                device_id=(freq, other),
                device_id_type=MESH,
            )
        )
    for copy in copies:
        copy.start()

    for field, ref in enumerate((receiver_ref, source_ref)):
        for part in range(2):
            fields[2 * field + part, rows : 2 * rows, :] = ref[part, 0]
    classes[rows : 2 * rows, :] = class_ref[...]
    for copy in copies:
        copy.wait()
    first = strip == 0
    last = strip == strips - 1
    for comp in range(4):
        above = rows_in[1, 2 * comp : 2 * comp + 2, :]
        below = rows_in[0, 2 * comp : 2 * comp + 2, :]
        fields[comp, rows - 2 : rows, :] = jnp.where(first, 0.0, above)
        fields[comp, 2 * rows : 2 * rows + 2, :] = jnp.where(last, 0.0, below)
    classes[rows - 1 : rows, :] = class_in[1]
    classes[2 * rows : 2 * rows + 1, :] = class_in[0]

    levels = classes[rows - 1 : 3 * rows - 1, :]
    for part in range(2):
        for tap in range(9):
            value = jnp.full(levels.shape, filters_ref[0, 0, part, tap], jnp.float32)
            for level in range(1, NCLASS):
                value = jnp.where(levels == level, filters_ref[0, level, part, tap], value)
            coefs[part * 9 + tap] = value

    edge = lax.broadcasted_iota(jnp.int32, (1, cols), 1)

    def shift_all():
        for comp in range(4):
            base = fields[comp]
            shifted[comp, 0] = jnp.where(edge == 0, 0.0, pltpu.roll(base, 1, 1))
            shifted[comp, 1] = base
            shifted[comp, 2] = jnp.where(edge == cols - 1, 0.0, pltpu.roll(base, cols - 1, 1))

    def advance(field, start, count, skip):
        factor = 1.0 if field == 0 else -1.0
        real_part = jnp.zeros((count, cols), jnp.float32)
        imag_part = jnp.zeros((count, cols), jnp.float32)
        for tap in range(9):
            at = start + tap // 3 - 1
            near_real = shifted[2 * field, tap % 3, at : at + count, :]
            near_imag = shifted[2 * field + 1, tap % 3, at : at + count, :]
            coef_real = coefs[tap, skip : skip + count, :]
            coef_imag = factor * coefs[9 + tap, skip : skip + count, :]
            real_part = real_part + coef_real * near_real - coef_imag * near_imag
            imag_part = imag_part + coef_real * near_imag + coef_imag * near_real
        return real_part, imag_part

    shift_all()
    line = lax.broadcasted_iota(jnp.int32, (2 * rows, cols), 0)
    alive = (line < rows + 2) & ((line > 0) | (strip > 0)) & ((line < rows + 1) | (strip < strips - 1))
    ahead = advance(0, rows - 1, 2 * rows, 0) + advance(1, rows - 1, 2 * rows, 0)
    for comp in range(4):
        fields[comp, rows - 1 : 3 * rows - 1, :] = jnp.where(alive, ahead[comp], 0.0)
    shift_all()
    second = advance(0, rows, rows, 1) + advance(1, rows, rows, 1)
    firsts = [fields[comp, rows : 2 * rows, :] for comp in range(4)]
    for depth, f in enumerate((firsts, second)):
        image = f[0] * f[2] + f[1] * f[3]
        for g in range(groups):
            terms[g, depth] = image[:, g * share : (g + 1) * share]

    def send_terms(i, carry):
        other = lax.rem(freq + i, groups)
        pltpu.make_async_remote_copy(
            src_ref=terms.at[other],
            dst_ref=terms_in.at[i - 1],
            send_sem=send_sem.at[2],
            recv_sem=recv_sem.at[2],
            device_id=(other, strip),
            device_id_type=MESH,
        ).start()
        return carry

    def wait_all(buffer, sem):
        pltpu.make_async_copy(buffer, buffer, sem).wait()

    lax.fori_loop(1, groups, send_terms, 0)
    wait_all(terms_in, recv_sem.at[2])
    scaling = 1.0 / math.sqrt(groups)
    migrated = terms[freq]
    for i in range(groups - 1):
        migrated = migrated + terms_in[i]
    migrated = migrated * scaling
    for depth in range(STEPS):
        migrated_ref[:, depth, :] = migrated[depth]

    quarter = share // 4
    half = share // 2
    slim = lax.broadcasted_iota(jnp.int32, (1, share), 1)

    def send_rim(value, turn):
        rim_out[turn] = value
        rim_in[turn, span - 1] = value
        far_round = pltpu.roll(value[1], half, 1)
        edge_out[turn] = jnp.where((slim >= quarter) & (slim < share - quarter), far_round, value[0])
        for dj, dk in reaches[:-1]:
            plain = dk == 0
            source = rim_out if plain else edge_out
            target = rim_in if plain else edge_in
            sem = rim_sem if plain else edge_sem
            slot = rim_place[-dj] if plain else edge_place[(-dj, -dk)]
            pltpu.make_async_remote_copy(
                src_ref=source.at[turn],
                dst_ref=target.at[turn, slot],
                send_sem=sem.at[2 * turn],
                recv_sem=sem.at[2 * turn + 1],
                device_id=(
                    lax.rem(freq + dk + groups, groups),
                    lax.rem(strip + dj + near * strips, strips),
                ),
                device_id_type=MESH,
            ).start()


    def send_sums(parts, turn):
        row = jnp.zeros((1, share), jnp.float32)
        for at, part in enumerate(parts):
            lanes = jnp.sum(part, axis=0, keepdims=True)
            lanes = lanes + pltpu.roll(lanes, share // 2, 1)
            lanes = lanes + pltpu.roll(lanes, quarter, 1)
            row = jnp.where((slim >= at * quarter) & (slim < (at + 1) * quarter), lanes, row)
        sums_out[turn] = row

        def send(i, carry):
            other = lax.rem(me + i, total)
            pltpu.make_async_remote_copy(
                src_ref=sums_out.at[turn],
                dst_ref=sums_in.at[turn, i - 1],
                send_sem=sum_sem.at[2 * turn],
                recv_sem=sum_sem.at[2 * turn + 1],
                device_id=(other // strips, lax.rem(other, strips)),
                device_id_type=MESH,
            ).start()
            return carry

        lax.fori_loop(1, total, send, 0)
        return row

    def take_sums(row, turn, count):
        wait_all(sums_in.at[turn], sum_sem.at[2 * turn + 1])
        row = row + jnp.sum(sums_in[turn], axis=0)
        return [
            jnp.sum(
                jnp.where((slim >= at * quarter) & (slim < (at + 1) * quarter), row, 0.0),
                axis=1,
                keepdims=True,
            )
            for at in range(count)
        ]

    def rim_values(turn):
        found = []
        for dj in range(-near, near + 1):
            ok = (strip + dj >= 0) & (strip + dj < strips)
            pair = []
            right = jnp.where(ok & (freq < groups - 1), edge_in[turn, edge_place[(dj, 1)]], 0.0)
            left = jnp.where(ok & (freq > 0), edge_in[turn, edge_place[(dj, -1)]], 0.0)
            both = jnp.where(lax.rem(slim, half) < quarter, right, left)
            for depth in range(STEPS):
                middle = jnp.where(ok, rim_in[turn, rim_place[dj], depth], 0.0)
                outer = both if depth == 0 else pltpu.roll(both, half, 1)
                outer = jnp.where((slim < 2 * reach) | (slim >= share - 2 * reach), outer, 0.0)
                pair.append(jnp.concatenate([middle, outer], axis=1))
            found.append(pair)
        return found

    tall = 3 * rows

    def descend(weighted):
        for j in range(span):
            for st in range(2):
                both = weighted[j][0] + weighted[j][1] if st == 0 else weighted[j][0] - weighted[j][1]
                for b in range(side):
                    rolled[2 * j + st, b] = pltpu.roll(both, (b - reach) % wide, 1)
        spill[...] = jnp.zeros_like(spill)

        base = near * rows

        def one(st, carry):
            for j in range(span):
                taps = [a for a in range(side) if base - rows < rows * j + a < base + rows + 2 * reach]
                for low in range(0, len(taps), 5):
                    some = taps[low : low + 5]
                    totals = [jnp.zeros((rows, wide), jnp.float32) for a in some]
                    for b in range(side):
                        data = rolled[2 * j + st, b]
                        for at, a in enumerate(some):
                            totals[at] = totals[at] + table[2 * j + st, b, a : a + 1, :] * data
                    for at, a in enumerate(some):
                        spill[st, rows * j + a : rows * j + a + rows, :] += totals[at]
            return carry

        lax.fori_loop(0, 2, one, 0)
        depth_line = lax.broadcasted_iota(jnp.int32, (tall, wide), 0) - reach + strip * rows
        at_col = column + freq * share
        ok = (
            (depth_line >= 0)
            & (depth_line < strips * rows)
            & (at_col >= 0)
            & (at_col < groups * share)
        )
        values = [jnp.where(ok, spill[st, base : base + tall, :], 0.0) for st in range(2)]
        for st in range(2):
            spill[st, base : base + tall, :] = values[st]
        mine = [spill[st, base + reach : base + reach + rows, 0:share] for st in range(2)]
        descent = [0.5 * (mine[0] + mine[1]), 0.5 * (mine[0] - mine[1])]
        image = [jnp.zeros((rows, share), jnp.float32) for st in range(2)]
        for st in range(2):
            for b in range(side):
                moved[st, b] = pltpu.roll(values[st], (reach - b) % wide, 1)[:, 0:share]
            for b in range(side):
                for a in range(side):
                    image[st] = image[st] + own_table[st, b, a : a + 1, :] * moved[st, b, a : a + rows, :]
        image_of = [0.5 * (image[0] + image[1]), 0.5 * (image[0] - image[1])]
        return descent, image_of

    cells = float(STEPS * rows * strips * cols)
    row = send_sums([migrated[0] * migrated[0] + migrated[1] * migrated[1]], 0)
    send_rim(-migrated, 0)
    wait_all(rim_in.at[0, 0 : span - 1], rim_sem.at[1])
    wait_all(edge_in.at[0], edge_sem.at[1])
    residual = rim_values(0)
    (energy,) = take_sums(row, 0, 1)
    reflect = [jnp.zeros((rows, share), jnp.float32) for depth in range(STEPS)]
    for turn in range(1, PASSES + 1):
        weights = [
            [1.0 / jnp.sqrt(r * r + energy / cells) for r in pair] for pair in residual
        ]
        weighted = [[w * r for w, r in zip(ws, rs)] for ws, rs in zip(weights, residual)]
        descent, image_of = descend(weighted)
        parts = [jnp.zeros((rows, share), jnp.float32) for q in range(4)]
        for depth in range(STEPS):
            v = image_of[depth]
            r = residual[near][depth][:, 0:share]
            w = weights[near][depth][:, 0:share]
            parts[0] = parts[0] + descent[depth] * descent[depth]
            parts[1] = parts[1] + w * v * v
            parts[2] = parts[2] + r * v
            parts[3] = parts[3] + v * v
        row = send_sums(parts, turn)
        if turn < PASSES:
            send_rim(jnp.stack(image_of), turn)
            wait_all(rim_in.at[turn, 0 : span - 1], rim_sem.at[2 * turn + 1])
            wait_all(edge_in.at[turn], edge_sem.at[2 * turn + 1])
            images = rim_values(turn)
        grad_square, curvature, cross_term, power_term = take_sums(row, turn, 4)
        step_length = grad_square / curvature
        energy = energy - 2.0 * step_length * cross_term + step_length * step_length * power_term
        reflect = [x - step_length * d for x, d in zip(reflect, descent)]
        if turn < PASSES:
            residual = [
                [r - step_length * v for r, v in zip(rs, vs)] for rs, vs in zip(residual, images)
            ]
    for depth in range(STEPS):
        reflect_ref[:, depth, :] = reflect[depth]
    misfit_ref[...] = energy / cells

    wait_all(terms_in, send_sem.at[2])
    for turn in range(PASSES):
        wait_all(rim_in.at[turn, 0 : span - 1], rim_sem.at[2 * turn])
        wait_all(edge_in.at[turn], edge_sem.at[2 * turn])
    for turn in range(PASSES + 1):
        wait_all(sums_in.at[turn], sum_sem.at[2 * turn])


def local(receiver_field, source_field, velocity_class, filters, point_spread, spread_index):
    groups = lax.axis_size("freq")
    strips = lax.axis_size("strip")
    rows, cols = velocity_class.shape
    share = cols // groups
    side = point_spread.shape[2]
    reach = side // 2
    near = -(-2 * reach // rows)
    total = groups * strips
    wide = 2 * share
    vmem = pl.BlockSpec(memory_space=pltpu.VMEM)
    smem = pl.BlockSpec(memory_space=pltpu.SMEM)
    f32 = jnp.float32
    dma = pltpu.SemaphoreType.DMA
    deep = -(-(rows * (2 * near + 1) + side) // 8) * 8
    migrated, reflectivity, misfit = pl.pallas_call(
        functools.partial(kernel, groups, strips, near),
        out_shape=(
            jax.ShapeDtypeStruct((rows, STEPS, share), f32),
            jax.ShapeDtypeStruct((rows, STEPS, share), f32),
            jax.ShapeDtypeStruct((1, 1), f32),
        ),
        in_specs=[smem, smem, vmem, vmem, vmem, vmem],
        out_specs=(vmem, vmem, vmem),
        scratch_shapes=[
            pltpu.VMEM((2, 8, cols), f32),
            pltpu.VMEM((2, 8, cols), f32),
            pltpu.VMEM((2, 1, cols), jnp.int32),
            pltpu.VMEM((2, 1, cols), jnp.int32),
            pltpu.VMEM((4, 3 * rows, cols), f32),
            pltpu.VMEM((3 * rows, cols), jnp.int32),
            pltpu.VMEM((4, 3, 3 * rows, cols), f32),
            pltpu.VMEM((18, 2 * rows, cols), f32),
            pltpu.VMEM((groups, STEPS, rows, share), f32),
            pltpu.VMEM((groups - 1, STEPS, rows, share), f32),
            pltpu.VMEM((2, side, 16, share), f32),
            pltpu.VMEM((2, side, 16, share), f32),
            pltpu.VMEM((2 * (2 * near + 1), side, 16, wide), f32),
            pltpu.VMEM((PASSES, STEPS, rows, share), f32),
            pltpu.VMEM((PASSES, 2 * near + 1, STEPS, rows, share), f32),
            pltpu.VMEM((PASSES, rows, share), f32),
            pltpu.VMEM((PASSES, 2 * (2 * near + 1), rows, share), f32),
            pltpu.VMEM((2 * (2 * near + 1), side, rows, wide), f32),
            pltpu.VMEM((2, deep, wide), f32),
            pltpu.VMEM((2, side, 3 * rows, share), f32),
            pltpu.VMEM((PASSES + 1, 1, share), f32),
            pltpu.VMEM((PASSES + 1, total - 1, 1, share), f32),
            dma((3,)),
            dma((3,)),
            dma((4,)),
            dma((2 * PASSES,)),
            dma((2 * PASSES,)),
            dma((2 * (PASSES + 1),)),
        ],
        compiler_params=pltpu.CompilerParams(collective_id=0, has_side_effects=True),
    )(
        spread_index.T,
        filters,
        receiver_field,
        source_field,
        velocity_class,
        jnp.transpose(point_spread, (2, 3, 1, 0)),
    )
    return migrated, reflectivity, misfit[0, 0]


def solution(mesh):
    return jax.shard_map(
        local,
        mesh=mesh,
        in_specs=(
            P(None, "freq", "strip", None),
            P(None, "freq", "strip", None),
            P("strip", None),
            P("freq", None, None, None),
            P(),
            P(),
        ),
        out_specs=(P("strip", None, "freq"), P("strip", None, "freq"), P()),
        check_vma=False,
    )
```
